256 devices in a mesh: expert: 32 (over x, z_hi, core), tensor: 8 (over y, z_lo).
Axes of the slice: x: 4, y: 4, z: 8 (z_hi: 4, z_lo: 2; z = z_hi * 2 + z_lo), core: 2. Of those that a mesh axis runs over, the one named last changes fastest.
Arguments:
- tokens: bfloat16 [512, 7168], P('expert'), may hold values from -6 to 6
- routes: int32 [512, 8], P('expert'), may hold values from 0 to 31, all different within a row; in each aligned block of 16 rows (0 to 15, 16 to 31, ...) at most 8 rows name the same one
- route_logits: float32 [512, 8], P('expert'), may hold values from -8 to 8
- gate_weight: bfloat16 [32, 7168, 1024], P('expert', 'tensor'), may hold values from -0.0625 to 0.0625
- up_weight: bfloat16 [32, 7168, 1024], P('expert', 'tensor'), may hold values from -0.0625 to 0.0625
- down_weight: bfloat16 [32, 7168, 1024], P('expert', 'tensor'), may hold values from -0.1875 to 0.1875
Outputs:
- mixed: bfloat16 [512, 7168], P('expert', 'tensor')
The draws below stay inside these ranges and needn't reach their ends.
Inputs may be any that keep to these rules, and one draw needn't show every extreme that they name: `routes`: each row names 8 different experts. In each aligned block of 16 rows (the rows of one index of expert) no expert is named by more than 8 rows, a bound that some block reaches.
All inputs are finite; a program needn't handle non-finite values.
Results may differ from the reference program's by a relative error of at most 0.0066.
Values may be sent and summed in bfloat16 or wider, within the bound.
No kernel may reach another device: no remote copies, remote signals or barrier semaphores. Data moves between devices by JAX's collectives and lax.ppermute only.
A program may use at most 64 MiB of HBM per device.

```python
import math
import jax
import jax.numpy as jnp
import numpy as np
from jax import lax

D = 7168
F = 1024
TOP = 8
TOK_DEV = 16
EXPERTS = 32
CAP = 8
TOKENS = 512


def block_scale(rng, dims, shards, low, top_value):
    level = 1.0
    for axis_at, shards_of in shards:
        steps = jax.random.uniform(jax.random.fold_in(jax.random.fold_in(rng, 6), axis_at), (shards_of,), jnp.float32, low / len(shards), top_value / len(shards))
        level = level * jnp.repeat(jnp.exp(steps), dims[axis_at] // shards_of).reshape((-1,) + (1,) * (len(dims) - 1 - axis_at))
    return level


def deal_out(key, own, number, rows, number_of, top, limit, skew):
    sequence = jax.random.permutation(key, number_of)
    crowded, usual = portions_of(number_of, rows * top, limit, skew, True), portions_of(number_of, rows * top, limit, skew, False)
    places = jnp.arange(number_of)

    def named(tallies, offset_by):
        used = int((tallies > 0).sum())
        fixed = max(1, used // 4)
        shifted = fixed + (places - fixed + offset_by * (used - fixed)) % max(1, number_of - fixed)
        return jnp.zeros((number_of,), jnp.int32).at[sequence[jnp.where(places < fixed, places, shifted)]].set(jnp.asarray(tallies, jnp.int32))

    tallies = jnp.where(number % 4 == 0, named(crowded, number // 4), named(usual, number - number // 4 - 1))
    mixed = jax.random.permutation(jax.random.fold_in(own, 3), number_of)
    donor, receiver = mixed[0:number_of // 2 * 2:2], mixed[1:number_of // 2 * 2:2]
    slack = jnp.minimum(tallies[donor] - 1, limit - tallies[receiver]) // 2
    slack = jnp.where((donor == sequence[0]) | (receiver == sequence[0]) | (tallies[receiver] == 0), 0, jnp.maximum(slack, 0))
    shifted = jax.random.randint(jax.random.fold_in(own, 4), (number_of // 2,), 0, 1 << 20) % (slack + 1)
    tallies = tallies.at[donor].add(-shifted).at[receiver].add(shifted)
    items = jnp.searchsorted(jnp.cumsum(tallies), jnp.arange(rows * top), side="right").astype(jnp.int32)
    listing = items.reshape(top, rows).T
    listing = listing[jax.random.permutation(jax.random.fold_in(own, 1), rows)]
    offset_by = jax.random.randint(jax.random.fold_in(own, 2), (rows, 1), 0, top)
    return jnp.take_along_axis(listing, (jnp.arange(top)[None, :] + offset_by) % top, axis=1)


def portions_of(count, total, limit, slope, full):
    loads = [(1 << 20) // math.isqrt(grade ** slope) + 1 for grade in range(1, count + 1)]
    largest = limit if full else min(limit, max(-(-total // count), total * loads[0] // sum(loads)))
    least = 1 if total - largest >= count - 1 else 0
    holding, surplus = [largest] + [least] * (count - 1), total - largest - least * (count - 1)
    while surplus > 0:
        free = [i for i in range(1, count) if holding[i] < largest] or [i for i in range(1, count) if holding[i] < limit]
        whole, remaining = sum([loads[i] for i in free]), surplus
        for i in free:
            more = min(limit - holding[i], max(1, remaining * loads[i] // whole), surplus)
            holding[i] = holding[i] + more
            surplus = surplus - more
    return np.array(holding)


def noise(rng, extent, deviation, limit, pieces=(), kind=jnp.bfloat16):
    drawn = deviation * jax.random.normal(rng, extent, jnp.float32)
    if pieces:
        drawn = drawn * block_scale(rng, extent, pieces, -0.22, 0.18)
    return jnp.clip(drawn, -limit, limit).astype(kind)


def setup_inputs(seed: int = 0) -> dict:
    seeds = jax.random.split(jax.random.key(seed), 7)
    tokens = noise(seeds[0], (TOKENS, D), 1.0, 6.0, ((0, 32),))
    routes_keys = jax.random.split(jax.random.fold_in(seeds[1], 1), TOKENS // TOK_DEV)
    routes_turns = jax.random.permutation(jax.random.fold_in(seeds[1], 3), TOKENS // TOK_DEV)
    routes = jax.vmap(lambda own, number: deal_out(jax.random.fold_in(seeds[1], 2), own, number, TOK_DEV, EXPERTS, TOP, CAP, 2))(routes_keys, routes_turns).reshape((TOKENS, TOP))
    route_logits = noise(seeds[2], (TOKENS, TOP), 2.0, 8.0, ((0, 32),), jnp.float32)
    gate_weight = noise(seeds[3], (EXPERTS, D, F), D ** -0.5, 0.0625, ((0, 32), (1, 8)))
    up_weight = noise(seeds[4], (EXPERTS, D, F), D ** -0.5, 0.0625, ((0, 32), (1, 8)))
    down_weight = noise(seeds[5], (EXPERTS, D, F), F ** -0.5, 0.1875, ((0, 32), (1, 8)))
    return {"tokens": tokens, "routes": routes, "route_logits": route_logits, "gate_weight": gate_weight, "up_weight": up_weight, "down_weight": down_weight}


routed_scale = 2.5


def reference(tokens, routes, route_logits, gate_weight, up_weight, down_weight):
    scores = jax.nn.sigmoid(route_logits)
    weights = routed_scale * scores / jnp.sum(scores, axis=1, keepdims=True)
    block_count = TOKENS // TOK_DEV
    flat_routes = routes.reshape(block_count, TOK_DEV * TOP).astype(jnp.int32)
    one_hot = (flat_routes[:, :, None] == jnp.arange(EXPERTS, dtype=jnp.int32)[None, None, :]).astype(jnp.int32)
    earlier = jnp.cumsum(one_hot, axis=1) - one_hot
    position = jnp.sum(earlier * one_hot, axis=2).astype(jnp.int32)
    block_ids = jnp.broadcast_to(jnp.arange(block_count, dtype=jnp.int32)[:, None], flat_routes.shape).astype(jnp.int32)
    token_ids = (block_ids * TOK_DEV + jnp.arange(TOK_DEV * TOP, dtype=jnp.int32)[None, :] // TOP).astype(jnp.int32)
    table = jnp.zeros((EXPERTS, block_count, CAP), jnp.int32).at[flat_routes, block_ids, position].set(token_ids)
    portions = jnp.zeros((EXPERTS, block_count, CAP), jnp.float32).at[flat_routes, block_ids, position].set(
        weights.reshape(block_count, TOK_DEV * TOP).astype(jnp.float32))

    def expert_step(accumulated, expert_item):
        gate_w, up_w, down_w, rows_at, portion = expert_item
        row_index = rows_at.reshape(-1).astype(jnp.int32)
        picked = tokens[row_index]
        gate_value = jnp.dot(picked, gate_w, preferred_element_type=jnp.float32)
        up_value = jnp.dot(picked, up_w, preferred_element_type=jnp.float32)
        hidden = (jax.nn.silu(gate_value) * up_value).astype(jnp.bfloat16)
        output = jnp.dot(hidden, down_w.T, preferred_element_type=jnp.float32)
        accumulated = accumulated.at[row_index].add(portion.reshape(-1)[:, None] * output)
        return accumulated, None

    start = jnp.zeros((TOKENS, D), jnp.float32)
    accumulated, _ = lax.scan(expert_step, start, (gate_weight, up_weight, down_weight, table, portions))
    return accumulated.astype(jnp.bfloat16)
```

```python
import jax
import jax.numpy as jnp
from jax import lax
from jax.experimental import pallas as pl
from jax.experimental.pallas import tpu as pltpu
from jax.sharding import Mesh, PartitionSpec as P


SCALE = 2.5
CHIPS = 16
CAP = 8
LANES = 128
BF = jnp.bfloat16
F32 = jnp.float32

VM = pl.BlockSpec(memory_space=pltpu.VMEM)
SM = pl.BlockSpec(memory_space=pltpu.SMEM)


def route_body(where, routes, logits, tokens, send, combine):
    count, top = routes.shape
    slots = send.shape[0]
    named = routes[...] ^ where[1]
    score = 1.0 / (1.0 + jnp.exp(-logits[...]))
    weight = SCALE * score / jnp.sum(score, axis=1, keepdims=True)
    lane = lax.broadcasted_iota(jnp.int32, (count, slots), 1)
    expert, place = lane // CAP, (lane % CAP).astype(F32)
    hits = jnp.zeros((count, slots), F32)
    shares = jnp.zeros((count, slots), F32)
    for k in range(top):
        hit = named[:, k : k + 1] == expert
        hits = jnp.where(hit, 1.0, hits)
        shares = jnp.where(hit, weight[:, k : k + 1], shares)
    earlier = (
        lax.broadcasted_iota(jnp.int32, (count, count), 1)
        < lax.broadcasted_iota(jnp.int32, (count, count), 0)
    ).astype(F32)
    position = jnp.dot(earlier.astype(BF), hits.astype(BF), preferred_element_type=F32)
    chosen = (hits > 0.5) & (position == place)
    picker = jnp.where(chosen, 1.0, 0.0).astype(BF)
    send[...] = lax.dot_general(
        picker, tokens[...], (((0,), (0,)), ((), ())), preferred_element_type=F32
    ).astype(BF)
    exact = jnp.where(chosen, shares, 0.0)
    high = exact.astype(BF)
    rest = exact - high.astype(F32)
    middle = rest.astype(BF)
    low = (rest - middle.astype(F32)).astype(BF)
    combine[0:count, :] = high
    combine[count : 2 * count, :] = middle
    combine[2 * count : 3 * count, :] = low


def route(where, routes, logits, tokens, narrow):
    count = tokens.shape[0]
    slots = 2 * CHIPS * CAP
    full = lambda i, w: (0, 0)
    return pl.pallas_call(
        route_body,
        out_shape=(
            jax.ShapeDtypeStruct((slots, narrow), BF),
            jax.ShapeDtypeStruct((3 * count, slots), BF),
        ),
        grid_spec=pltpu.PrefetchScalarGridSpec(
            num_scalar_prefetch=1,
            grid=(1,),
            in_specs=[
                pl.BlockSpec(routes.shape, full),
                pl.BlockSpec(logits.shape, full),
                pl.BlockSpec((count, narrow), lambda i, w: (0, w[0])),
            ],
            out_specs=[
                pl.BlockSpec((slots, narrow), full),
                pl.BlockSpec((3 * count, slots), full),
            ],
        ),
        name="route",
    )(where, routes, logits, tokens)


def up_body(where, own, other, gate, up, *outs):
    rows = jnp.concatenate([own[...], other[...]], axis=0)
    for k, out in enumerate(outs):
        at = pl.multiple_of((where[0] ^ k) * LANES, LANES)
        both = jnp.concatenate([gate[:, pl.ds(at, LANES)], up[:, pl.ds(at, LANES)]], axis=1)
        out[...] = jnp.dot(rows, both, preferred_element_type=F32).astype(out.dtype)


def up_parts(where, own, other, gate, up, shards):
    rows = own.shape[0] + other.shape[0]
    return pl.pallas_call(
        up_body,
        out_shape=[
            jax.ShapeDtypeStruct((rows, 2 * LANES), F32 if k == 0 else BF) for k in range(shards)
        ],
        in_specs=[SM, VM, VM, VM, VM],
        out_specs=[VM] * shards,
        name="gateup",
    )(where, own, other, gate, up)


def hidden_body(*refs):
    *parts, out = refs
    total = parts[0][...]
    for part in parts[1:]:
        total = total + part[...].astype(F32)
    gate, up = total[:, :LANES], total[:, LANES:]
    hidden = (gate / (1.0 + jnp.exp(-gate)) * up).astype(BF)
    for k in range(out.shape[0]):
        out[k] = hidden


def hidden_copies(parts, shards):
    rows = parts[0].shape[0]
    return pl.pallas_call(
        hidden_body,
        out_shape=jax.ShapeDtypeStruct((shards, rows, LANES), BF),
        in_specs=[VM] * len(parts),
        out_specs=VM,
        name="hidden",
    )(*parts)


def down_body(hidden, down, own, other):
    wide = jnp.concatenate([hidden[k] for k in range(hidden.shape[0])], axis=1)
    result = lax.dot_general(
        wide, down[...], (((1,), (1,)), ((), ())), preferred_element_type=F32
    ).astype(BF)
    half = own.shape[0]
    own[...] = result[:half]
    other[...] = result[half:]


def down_rows(hidden, down):
    half = jax.ShapeDtypeStruct((hidden.shape[1] // 2, down.shape[0]), BF)
    return pl.pallas_call(
        down_body,
        out_shape=(half, half),
        in_specs=[VM, VM],
        out_specs=(VM, VM),
        name="down",
    )(hidden, down)


def mix_body(returned, combine, out):
    count = out.shape[0]
    rows = returned[...]
    high = jnp.dot(combine[0:count], rows, preferred_element_type=F32)
    middle = jnp.dot(combine[count : 2 * count], rows, preferred_element_type=F32)
    low = jnp.dot(combine[2 * count :], rows, preferred_element_type=F32)
    out[...] = (high + (middle + low)).astype(BF)


def mix(returned, combine):
    return pl.pallas_call(
        mix_body,
        out_shape=jax.ShapeDtypeStruct((combine.shape[0] // 3, returned.shape[1]), BF),
        in_specs=[VM, VM],
        out_specs=VM,
        name="mix",
    )(returned, combine)


def shards(tokens, routes, route_logits, gate_weight, up_weight, down_weight):
    tensor = ("y", "z_lo")
    chips = ("x", "z_hi")
    shard_count = 8
    width = tokens.shape[1]
    narrow = width // shard_count
    core = lax.axis_index("core")
    where = jnp.stack([lax.axis_index(tensor), core]).astype(jnp.int32)
    swap = [(0, 1), (1, 0)]
    gate, up, down = gate_weight[0], up_weight[0], down_weight[0]

    send, combine = route(where, routes, route_logits, tokens, narrow)
    arrived = lax.all_to_all(
        send.reshape(CHIPS, 2 * CAP, narrow), chips, split_axis=0, concat_axis=0, tiled=True
    ).reshape(CHIPS, 2, CAP, narrow)
    own = arrived[:, 0].reshape(CHIPS * CAP, narrow)
    other = lax.ppermute(arrived[:, 1].reshape(CHIPS * CAP, narrow), "core", swap)

    parts = up_parts(where, own, other, gate, up, shard_count)
    landed = [parts[0]] + [
        lax.ppermute(parts[k], tensor, [(j, j ^ k) for j in range(shard_count)])
        for k in range(1, shard_count)
    ]
    copies = hidden_copies(landed, shard_count)
    hidden = lax.all_to_all(copies, tensor, split_axis=0, concat_axis=0, tiled=True)
    own, other = down_rows(hidden, down)
    other = lax.ppermute(other, "core", swap)
    back = jnp.stack(
        [own.reshape(CHIPS, CAP, narrow), other.reshape(CHIPS, CAP, narrow)], axis=1
    ).reshape(CHIPS, 2 * CAP, narrow)
    returned = lax.all_to_all(back, chips, split_axis=0, concat_axis=0, tiled=True)
    return mix(returned.reshape(2 * CHIPS * CAP, narrow), combine)


def solution(mesh):
    wide = Mesh(mesh.devices.reshape(4, 4, 2, 4, 2), ("x", "z_hi", "core", "y", "z_lo"))
    expert, tensor = ("x", "z_hi", "core"), ("y", "z_lo")
    return jax.shard_map(
        shards,
        mesh=wide,
        in_specs=(
            P(expert, None),
            P(expert, None),
            P(expert, None),
            P(expert, tensor, None),
            P(expert, tensor, None),
            P(expert, tensor, None),
        ),
        out_specs=P(expert, tensor),
        check_vma=False,
    )
```

```python
import jax
import jax.numpy as jnp
from jax import lax
from jax.experimental import pallas as pl
from jax.experimental.pallas import tpu as pltpu
from jax.sharding import Mesh, PartitionSpec as P


SCALE = 2.5
CHIPS = 16
CAP = 8
LANES = 128
BF = jnp.bfloat16
F32 = jnp.float32
FAR = ((2, BF), (1, BF), (3, BF), (0, F32))
NEAR = ((1, BF), (3, BF), (2, F32), (0, F32))

VM = pl.BlockSpec(memory_space=pltpu.VMEM)
HB = pl.BlockSpec(memory_space=pltpu.HBM)
SM = pl.BlockSpec(memory_space=pltpu.SMEM)


def in_vmem(array):
    return pltpu.with_memory_space_constraint(array, pltpu.VMEM)


def in_hbm(array):
    return pltpu.with_memory_space_constraint(array, pltpu.HBM)


def kernel(body, name, mib, **settings):
    return pl.pallas_call(
        body,
        compiler_params=pltpu.CompilerParams(vmem_limit_bytes=mib << 20),
        name=name,
        **settings,
    )


def fetches(start, gate, up, fetched, sems):
    half = fetched.shape[2]
    return [
        pltpu.make_async_copy(
            weight.at[:, pl.ds(pl.multiple_of(start * half, LANES), half)], fetched.at[j], sems.at[j]
        )
        for j, weight in enumerate((gate, up))
    ]


def route_body(
    where, routes, logits, tokens, gate, up, send, combine, fetched,
    columns, chosen_routes, raw, sems, weight_sems,
):
    top, count = routes.shape
    slots, narrow = send.shape
    start = pl.multiple_of(where[0] * narrow, LANES)
    loads = [
        pltpu.make_async_copy(routes, chosen_routes, sems.at[0]),
        pltpu.make_async_copy(logits, raw, sems.at[1]),
        pltpu.make_async_copy(tokens.at[:, pl.ds(start, narrow)], columns, sems.at[2]),
    ]
    for load in loads:
        load.start()
    later = fetches(1 - where[3], gate, up, fetched, weight_sems)
    for load in later:
        load.start()
    for load in loads:
        load.wait()
    named = chosen_routes[...] ^ where[1]
    score = 1.0 / (1.0 + jnp.exp(-raw[...]))
    weight = SCALE * score / jnp.sum(score, axis=0, keepdims=True)
    slot = lax.broadcasted_iota(jnp.int32, (slots, count), 0)
    expert, place = slot // CAP, (slot % CAP).astype(F32)
    hits = jnp.zeros((slots, count), F32)
    shares = jnp.zeros((slots, count), F32)
    for k in range(top):
        hit = named[k : k + 1, :] == expert
        hits = jnp.where(hit, 1.0, hits)
        shares = jnp.where(hit, weight[k : k + 1, :], shares)
    earlier = (
        lax.broadcasted_iota(jnp.int32, (count, count), 0)
        < lax.broadcasted_iota(jnp.int32, (count, count), 1)
    ).astype(F32)
    position = jnp.dot(hits.astype(BF), earlier.astype(BF), preferred_element_type=F32)
    chosen = (hits > 0.5) & (position == place)
    picker = jnp.where(chosen, 1.0, 0.0).astype(BF)
    send[...] = jnp.dot(picker, columns[...], preferred_element_type=F32).astype(BF)
    exact = jnp.where(chosen, shares, 0.0)
    high = exact.astype(BF)
    rest = exact - high.astype(F32)
    middle = rest.astype(BF)
    combine[0] = high
    combine[1] = middle
    combine[2] = (rest - middle.astype(F32)).astype(BF)
    for load in later:
        load.wait()


def route(where, routes, logits, tokens, gate, up):
    count = tokens.shape[0]
    narrow = gate.shape[0]
    slots = 2 * CHIPS * CAP
    return kernel(
        route_body,
        "route",
        4,
        out_shape=(
            pltpu.VMEM((slots, narrow), BF),
            pltpu.VMEM((3, slots, count), BF),
            pltpu.VMEM((2, narrow, gate.shape[1] // 2), BF),
        ),
        in_specs=[SM, HB, HB, HB, HB, HB],
        out_specs=(VM, VM, VM),
        scratch_shapes=[
            pltpu.VMEM((count, narrow), BF),
            pltpu.VMEM(routes.shape, jnp.int32),
            pltpu.VMEM(logits.shape, F32),
            pltpu.SemaphoreType.DMA((3,)),
            pltpu.SemaphoreType.DMA((2,)),
        ],
    )(where, in_hbm(routes), in_hbm(logits), in_hbm(tokens), in_hbm(gate), in_hbm(up))


def split_body(arrived, out):
    out[...] = arrived[:, 1]


def split(arrived):
    chips, _, cap, narrow = arrived.shape
    return kernel(
        split_body,
        "split",
        4,
        out_shape=pltpu.VMEM((chips, cap, narrow), BF),
        in_specs=[VM],
        out_specs=VM,
    )(in_vmem(arrived))


def merge_body(own, other, out):
    out[:, 0] = own[...]
    out[:, 1] = other[...]


def merge(own, other):
    chips, cap, narrow = own.shape
    return kernel(
        merge_body,
        "merge",
        4,
        out_shape=pltpu.VMEM((chips, 2, cap, narrow), BF),
        in_specs=[VM, VM],
        out_specs=VM,
    )(in_vmem(own), in_vmem(other))


def gathered_rows(arrived, other):
    chips, cap, narrow = other.shape
    own = arrived[:, 0].reshape(chips * cap, narrow)
    return jnp.concatenate([own, other[...].reshape(chips * cap, narrow)], axis=0)


def multiply(where, rows, weights, outs, steps):
    for (dy, _), out in zip(steps, outs):
        at = pl.multiple_of((where[2] + dy) % 4 * LANES, LANES)
        both = jnp.concatenate([weights[j, :, pl.ds(at, LANES)] for j in range(2)], axis=1)
        out[...] = jnp.dot(rows, both, preferred_element_type=F32).astype(out.dtype)


def far_body(where, arrived, other, weights, gate, up, *rest):
    *outs, fetched, sems = rest
    later = fetches(where[3], gate, up, fetched, sems)
    for load in later:
        load.start()
    multiply(where, gathered_rows(arrived, other), weights, outs, FAR)
    for load in later:
        load.wait()


def near_body(where, arrived, other, weights, *outs):
    multiply(where, gathered_rows(arrived, other), weights, outs, NEAR)


def far_parts(where, arrived, other, weights, gate, up):
    rows = 2 * other.shape[0] * other.shape[1]
    return kernel(
        far_body,
        "far",
        8,
        out_shape=[pltpu.VMEM((rows, 2 * LANES), kind) for _, kind in FAR]
        + [pltpu.VMEM(weights.shape, BF)],
        in_specs=[SM, VM, VM, VM, HB, HB],
        out_specs=[VM] * 5,
        scratch_shapes=[pltpu.SemaphoreType.DMA((2,))],
    )(where, in_vmem(arrived), in_vmem(other), in_vmem(weights), in_hbm(gate), in_hbm(up))


def near_parts(where, arrived, other, weights):
    rows = 2 * other.shape[0] * other.shape[1]
    return kernel(
        near_body,
        "near",
        8,
        out_shape=[pltpu.VMEM((rows, 2 * LANES), kind) for _, kind in NEAR],
        in_specs=[SM, VM, VM, VM],
        out_specs=[VM] * 4,
    )(where, in_vmem(arrived), in_vmem(other), in_vmem(weights))


def total_of(parts):
    total = parts[0][...].astype(F32)
    for part in parts[1:]:
        total = total + part[...].astype(F32)
    return total


def sum_body(*refs):
    *parts, out = refs
    out[...] = total_of(parts).astype(BF)


def summed(parts):
    return kernel(
        sum_body,
        "sum",
        4,
        out_shape=pltpu.VMEM(parts[0].shape, BF),
        in_specs=[VM] * len(parts),
        out_specs=VM,
    )(*[in_vmem(part) for part in parts])


def hidden_body(*refs):
    *parts, out = refs
    total = total_of(parts)
    gate, up = total[:, :LANES], total[:, LANES:]
    hidden = (gate / (1.0 + jnp.exp(-gate)) * up).astype(BF)
    for k in range(out.shape[0]):
        out[k] = hidden


def hidden_units(parts):
    return kernel(
        hidden_body,
        "hidden",
        4,
        out_shape=pltpu.VMEM((8, parts[0].shape[0], LANES), BF),
        in_specs=[VM] * len(parts),
        out_specs=VM,
    )(*[in_vmem(part) for part in parts])


def down_body(hidden, down, own, other):
    wide = jnp.concatenate([hidden[k] for k in range(8)], axis=1)
    result = lax.dot_general(
        wide, down[...], (((1,), (1,)), ((), ())), preferred_element_type=F32
    ).astype(BF)
    half = own.shape[0]
    own[...] = result[:half]
    other[...] = result[half:]


def down_rows(hidden, down):
    half = pltpu.VMEM((hidden.shape[1] // 2, down.shape[0]), BF)
    return kernel(
        down_body,
        "down",
        8,
        out_shape=(half, half),
        in_specs=[VM, VM],
        out_specs=(VM, VM),
    )(in_vmem(hidden), in_vmem(down))


def mix_body(returned, combine, out):
    rows = returned[...]
    high, middle, low = [
        lax.dot_general(
            combine[k], rows, (((0,), (0,)), ((), ())), preferred_element_type=F32
        )
        for k in range(3)
    ]
    out[...] = (high + (middle + low)).astype(BF)


def mix(returned, combine):
    return pl.pallas_call(
        mix_body,
        out_shape=jax.ShapeDtypeStruct((combine.shape[2], returned.shape[1]), BF),
        in_specs=[VM, VM],
        out_specs=VM,
        compiler_params=pltpu.CompilerParams(vmem_limit_bytes=4 << 20),
        name="mix",
    )(in_vmem(returned), in_vmem(combine))


def shards(tokens, routes, route_logits, gate_weight, up_weight, down_weight):
    chips = ("x", "z_hi")
    narrow = gate_weight.shape[1]
    core = lax.axis_index("core")
    where = [lax.axis_index(("y", "z_lo")), core, lax.axis_index("y"), lax.axis_index("z_lo")]
    where = jnp.stack(where).astype(jnp.int32)
    swap = [(0, 1), (1, 0)]
    gate, up, down = gate_weight[0], up_weight[0], down_weight[0]

    send, combine, weights = route(where, routes.T, route_logits.T, tokens, gate, up)
    arrived = lax.all_to_all(
        send.reshape(CHIPS, 2 * CAP, narrow), chips, split_axis=0, concat_axis=0, tiled=True
    ).reshape(CHIPS, 2, CAP, narrow)
    other = lax.ppermute(split(arrived), "core", swap)

    def along_y(array, dy):
        return lax.ppermute(array, "y", [(j, (j + dy) % 4) for j in range(4)])

    def across_z(array):
        return lax.ppermute(array, "z_lo", swap)

    far2, far1, far3, far0, weights = far_parts(where, arrived, other, weights, gate, up)
    crossed = across_z(far2)
    far1, far3 = along_y(far1, 1), along_y(far3, 3)
    near1, near3, near2, near0 = near_parts(where, arrived, other, weights)
    near1, near3 = along_y(near1, 1), along_y(near3, 3)
    near2 = along_y(summed([near2, crossed]), 2)
    relayed = across_z(summed([far0, far1, far3]))
    copies = hidden_units([near0, near1, near3, near2, relayed])
    hidden = lax.all_to_all(copies, ("z_lo", "y"), split_axis=0, concat_axis=0, tiled=True)
    own, other = down_rows(hidden, down)
    own, other = down_rows(hidden, down)
    other = lax.ppermute(other, "core", swap)
    back = merge(
        own.reshape(CHIPS, CAP, narrow), other.reshape(CHIPS, CAP, narrow)
    ).reshape(CHIPS, 2 * CAP, narrow)
    returned = lax.all_to_all(back, chips, split_axis=0, concat_axis=0, tiled=True)
    return mix(returned.reshape(2 * CHIPS * CAP, narrow), combine)


def solution(mesh):
    wide = Mesh(mesh.devices.reshape(4, 4, 2, 4, 2), ("x", "z_hi", "core", "y", "z_lo"))
    expert, tensor = ("x", "z_hi", "core"), ("y", "z_lo")
    return jax.shard_map(
        shards,
        mesh=wide,
        in_specs=(
            P(expert, None),
            P(expert, None),
            P(expert, None),
            P(expert, tensor, None),
            P(expert, tensor, None),
            P(expert, tensor, None),
        ),
        out_specs=P(expert, tensor),
        check_vma=False,
    )
```

```python
import jax
import jax.numpy as jnp
from jax import lax
from jax.experimental import pallas as pl
from jax.experimental.pallas import tpu as pltpu
from jax.sharding import Mesh, PartitionSpec as P


SCALE = 2.5
CHIPS = 16
CAP = 8
LANES = 128
BF = jnp.bfloat16
F32 = jnp.float32
FAR = ((2, BF), (1, BF), (3, BF), (0, F32))
NEAR = ((1, BF), (3, BF), (2, F32), (0, F32))

VM = pl.BlockSpec(memory_space=pltpu.VMEM)
HB = pl.BlockSpec(memory_space=pltpu.HBM)
SM = pl.BlockSpec(memory_space=pltpu.SMEM)


def in_vmem(array):
    return pltpu.with_memory_space_constraint(array, pltpu.VMEM)


def in_hbm(array):
    return pltpu.with_memory_space_constraint(array, pltpu.HBM)


def kernel(body, name, mib, **settings):
    return pl.pallas_call(
        body,
        compiler_params=pltpu.CompilerParams(vmem_limit_bytes=mib << 20),
        name=name,
        **settings,
    )


def route_body(
    where, routes, logits, tokens, up, own, other, combine, far_up, columns, chosen_routes, raw, sems
):
    top, count = routes.shape
    slots, narrow = 2 * CHIPS * CAP, own.shape[2]
    half = far_up.shape[1]
    far_start = pl.multiple_of((1 - where[3]) * half, LANES)
    start = pl.multiple_of(where[0] * narrow, LANES)
    loads = [
        pltpu.make_async_copy(routes, chosen_routes, sems.at[0]),
        pltpu.make_async_copy(logits, raw, sems.at[1]),
        pltpu.make_async_copy(tokens.at[:, pl.ds(start, narrow)], columns, sems.at[2]),
        pltpu.make_async_copy(up.at[:, pl.ds(far_start, half)], far_up, sems.at[3]),
    ]
    for load in loads:
        load.start()
    for load in loads[:2]:
        load.wait()
    named = chosen_routes[...] ^ where[1]
    score = 1.0 / (1.0 + jnp.exp(-raw[...]))
    weight = SCALE * score / jnp.sum(score, axis=0, keepdims=True)
    slot = lax.broadcasted_iota(jnp.int32, (slots, count), 0)
    expert, place = slot // CAP, (slot % CAP).astype(F32)
    hits = jnp.zeros((slots, count), F32)
    shares = jnp.zeros((slots, count), F32)
    for k in range(top):
        hit = named[k : k + 1, :] == expert
        hits = jnp.where(hit, 1.0, hits)
        shares = jnp.where(hit, weight[k : k + 1, :], shares)
    earlier = (
        lax.broadcasted_iota(jnp.int32, (count, count), 0)
        < lax.broadcasted_iota(jnp.int32, (count, count), 1)
    ).astype(F32)
    position = jnp.dot(hits.astype(BF), earlier.astype(BF), preferred_element_type=F32)
    chosen = (hits > 0.5) & (position == place)
    picker = jnp.where(chosen, 1.0, 0.0).astype(BF)
    loads[2].wait()
    picked = jnp.dot(picker, columns[...], preferred_element_type=F32)
    picked = picked.reshape(CHIPS, 2, CAP, narrow)
    own[...] = picked[:, 0].astype(BF)
    other[...] = picked[:, 1].astype(BF)
    exact = jnp.where(chosen, shares, 0.0)
    high = exact.astype(BF)
    rest = exact - high.astype(F32)
    middle = rest.astype(BF)
    for k, term in enumerate((high, middle, (rest - middle.astype(F32)).astype(BF))):
        paired = term.astype(F32).reshape(CHIPS, 2, CAP, count)
        for r in range(2):
            combine[k, r] = paired[:, r].reshape(CHIPS * CAP, count).astype(BF)
    loads[3].wait()


def route(where, routes, logits, tokens, up):
    count = tokens.shape[0]
    narrow, units = up.shape
    slots = 2 * CHIPS * CAP
    return kernel(
        route_body,
        "route",
        4,
        out_shape=(
            pltpu.VMEM((CHIPS, CAP, narrow), BF),
            pltpu.VMEM((CHIPS, CAP, narrow), BF),
            pltpu.VMEM((3, 2, slots // 2, count), BF),
            pltpu.VMEM((narrow, units // 2), BF),
        ),
        in_specs=[SM, HB, HB, HB, HB],
        out_specs=(VM, VM, VM, VM),
        scratch_shapes=[
            pltpu.VMEM((count, narrow), BF),
            pltpu.VMEM(routes.shape, jnp.int32),
            pltpu.VMEM(logits.shape, F32),
            pltpu.SemaphoreType.DMA((4,)),
        ],
    )(where, in_hbm(routes), in_hbm(logits), in_hbm(tokens), in_hbm(up))


def split_body(arrived, out):
    out[...] = arrived[:, 1]


def split(arrived):
    chips, _, cap, narrow = arrived.shape
    return kernel(
        split_body,
        "split",
        4,
        out_shape=pltpu.VMEM((chips, cap, narrow), BF),
        in_specs=[VM],
        out_specs=VM,
    )(in_vmem(arrived))


def merge_body(own, other, out):
    out[:, 0] = own[...]
    out[:, 1] = other[...]


def merge(own, other):
    chips, cap, narrow = own.shape
    return kernel(
        merge_body,
        "merge",
        4,
        out_shape=pltpu.VMEM((chips, 2, cap, narrow), BF),
        in_specs=[VM, VM],
        out_specs=VM,
    )(in_vmem(own), in_vmem(other))


def gathered_rows(arrived):
    chips, _, cap, narrow = arrived.shape
    return jnp.concatenate(
        [arrived[:, r].reshape(chips * cap, narrow) for r in range(2)], axis=0
    )


def multiply(where, rows, weights, outs, steps, held):
    for j, weight in enumerate(weights):
        result = jnp.dot(rows, weight, preferred_element_type=F32)
        for y in range(4):
            held[y, :, j * LANES : (j + 1) * LANES] = result[:, y * LANES : (y + 1) * LANES]
    for (dy, _), out in zip(steps, outs):
        out[...] = held[(where[2] + dy) % 4].astype(out.dtype)


def far_body(where, arrived, gate, far_up, *rest):
    *outs, held = rest
    rows = gathered_rows(arrived)
    half = far_up.shape[1]
    for parity in range(2):

        @pl.when(where[3] == parity)
        def _():
            start = (1 - parity) * half
            weights = gate[:, start : start + half], far_up[...]
            multiply(where, rows, weights, outs, FAR, held)


def near_body(where, arrived, gate, up, *rest):
    *outs, held = rest
    rows = gathered_rows(arrived)
    half = gate.shape[1] // 2
    for parity in range(2):

        @pl.when(where[3] == parity)
        def _():
            start = parity * half
            weights = gate[:, start : start + half], up[:, start : start + half]
            multiply(where, rows, weights, outs, NEAR, held)


def far_parts(where, arrived, gate, up):
    rows = 2 * CHIPS * CAP
    return kernel(
        far_body,
        "far",
        8,
        out_shape=[pltpu.VMEM((rows, 2 * LANES), kind) for _, kind in FAR],
        in_specs=[SM, VM, VM, VM],
        out_specs=[VM] * 4,
        scratch_shapes=[pltpu.VMEM((4, rows, 2 * LANES), F32)],
    )(where, in_vmem(arrived), in_vmem(gate), in_vmem(up))


def near_parts(where, arrived, gate, up):
    rows = 2 * CHIPS * CAP
    return kernel(
        near_body,
        "near",
        8,
        out_shape=[pltpu.VMEM((rows, 2 * LANES), kind) for _, kind in NEAR],
        in_specs=[SM, VM, VM, VM],
        out_specs=[VM] * 4,
        scratch_shapes=[pltpu.VMEM((4, rows, 2 * LANES), F32)],
    )(where, in_vmem(arrived), in_vmem(gate), in_vmem(up))


def total_of(parts):
    total = parts[0][...].astype(F32)
    for part in parts[1:]:
        total = total + part[...].astype(F32)
    return total


def sum_body(*refs):
    *parts, out = refs
    out[...] = total_of(parts).astype(BF)


def summed(parts):
    return kernel(
        sum_body,
        "sum",
        4,
        out_shape=pltpu.VMEM(parts[0].shape, BF),
        in_specs=[VM] * len(parts),
        out_specs=VM,
    )(*[in_vmem(part) for part in parts])


def hidden_body(*refs):
    *parts, out = refs
    total = total_of(parts)
    gate, up = total[:, :LANES], total[:, LANES:]
    hidden = (gate / (1.0 + jnp.exp(-gate)) * up).astype(BF)
    for k in range(out.shape[0]):
        out[k] = hidden


def hidden_units(parts):
    return kernel(
        hidden_body,
        "hidden",
        4,
        out_shape=pltpu.VMEM((8, parts[0].shape[0], LANES), BF),
        in_specs=[VM] * len(parts),
        out_specs=VM,
    )(*[in_vmem(part) for part in parts])


def down_body(hidden, down, out):
    wide = jnp.concatenate([hidden[k] for k in range(8)], axis=1)
    result = lax.dot_general(
        wide, down[...], (((1,), (1,)), ((), ())), preferred_element_type=F32
    ).astype(BF)
    half = result.shape[0] // 2
    for r in range(2):
        out[:, r] = result[r * half : (r + 1) * half].reshape(CHIPS, CAP, result.shape[1])


def down_rows(hidden, down):
    return kernel(
        down_body,
        "down",
        8,
        out_shape=pltpu.VMEM((CHIPS, 2, CAP, down.shape[0]), BF),
        in_specs=[VM, VM],
        out_specs=VM,
    )(in_vmem(hidden), in_vmem(down))


def weighted(combine, r, rows):
    rows = rows.reshape(CHIPS * CAP, rows.shape[2])
    high, middle, low = [
        lax.dot_general(
            combine[k, r], rows, (((0,), (0,)), ((), ())), preferred_element_type=F32
        )
        for k in range(3)
    ]
    return high + (middle + low)


def own_mix_body(back, combine, out):
    out[...] = weighted(combine, 0, back[:, 0])


def own_mix(back, combine):
    return kernel(
        own_mix_body,
        "own_mix",
        4,
        out_shape=pltpu.VMEM((combine.shape[3], back.shape[3]), F32),
        in_specs=[VM, VM],
        out_specs=VM,
    )(in_vmem(back), in_vmem(combine))


def mix_body(partial, other, combine, out):
    out[...] = (partial[...] + weighted(combine, 1, other[...])).astype(BF)


def mix(partial, other, combine):
    return kernel(
        mix_body,
        "mix",
        4,
        out_shape=jax.ShapeDtypeStruct(partial.shape, BF),
        in_specs=[VM, VM, VM],
        out_specs=VM,
    )(in_vmem(partial), in_vmem(other), in_vmem(combine))


def shards(tokens, routes, route_logits, gate_weight, up_weight, down_weight):
    chips = ("x", "z_hi")
    narrow = gate_weight.shape[1]
    core = lax.axis_index("core")
    where = [lax.axis_index(("y", "z_lo")), core, lax.axis_index("y"), lax.axis_index("z_lo")]
    where = jnp.stack(where).astype(jnp.int32)
    swap = [(0, 1), (1, 0)]
    gate, up, down = gate_weight[0], up_weight[0], down_weight[0]

    own, other, combine, far_up = route(where, routes.T, route_logits.T, tokens, up)
    rows = merge(own, lax.ppermute(other, "core", swap)).reshape(CHIPS, 2 * CAP, narrow)
    arrived = lax.all_to_all(
        rows, chips, split_axis=0, concat_axis=0, tiled=True
    ).reshape(CHIPS, 2, CAP, narrow)

    def along_y(array, dy):
        return lax.ppermute(array, "y", [(j, (j + dy) % 4) for j in range(4)])

    def across_z(array):
        return lax.ppermute(array, "z_lo", swap)

    far2, far1, far3, far0 = far_parts(where, arrived, gate, far_up)
    crossed = across_z(far2)
    far1, far3 = along_y(far1, 1), along_y(far3, 3)
    near1, near3, near2, near0 = near_parts(where, arrived, gate, up)
    near1, near3 = along_y(near1, 1), along_y(near3, 3)
    near2 = along_y(summed([near2, crossed]), 2)
    relayed = across_z(summed([far0, far1, far3]))
    copies = hidden_units([near0, near1, near3, near2, relayed])
    hidden = lax.all_to_all(copies, ("z_lo", "y"), split_axis=0, concat_axis=0, tiled=True)
    back = lax.all_to_all(
        down_rows(hidden, down).reshape(CHIPS, 2 * CAP, narrow),
        chips, split_axis=0, concat_axis=0, tiled=True,
    ).reshape(CHIPS, 2, CAP, narrow)
    other = lax.ppermute(split(back), "core", swap)
    return mix(own_mix(back, combine), other, combine)


def solution(mesh):
    wide = Mesh(mesh.devices.reshape(4, 4, 2, 4, 2), ("x", "z_hi", "core", "y", "z_lo"))
    expert, tensor = ("x", "z_hi", "core"), ("y", "z_lo")
    return jax.shard_map(
        shards,
        mesh=wide,
        in_specs=(
            P(expert, None),
            P(expert, None),
            P(expert, None),
            P(expert, tensor, None),
            P(expert, tensor, None),
            P(expert, tensor, None),
        ),
        out_specs=P(expert, tensor),
        check_vma=False,
    )
```

```python
import jax
import jax.numpy as jnp
from jax import lax
from jax.experimental import pallas as pl
from jax.experimental.pallas import tpu as pltpu
from jax.sharding import Mesh, PartitionSpec as P


SCALE = 2.5
CHIPS = 16
CAP = 8
LANES = 128
BF = jnp.bfloat16
F32 = jnp.float32
FAR = ((2, BF), (1, BF), (3, BF), (0, F32))
NEAR = ((1, BF), (3, BF), (2, F32), (0, F32))

VM = pl.BlockSpec(memory_space=pltpu.VMEM)
HB = pl.BlockSpec(memory_space=pltpu.HBM)
SM = pl.BlockSpec(memory_space=pltpu.SMEM)


def in_vmem(array):
    return pltpu.with_memory_space_constraint(array, pltpu.VMEM)


def in_hbm(array):
    return pltpu.with_memory_space_constraint(array, pltpu.HBM)


def kernel(body, name, mib, **settings):
    return pl.pallas_call(
        body,
        compiler_params=pltpu.CompilerParams(vmem_limit_bytes=mib << 20),
        name=name,
        **settings,
    )


def position_of():
    y, z_lo = lax.axis_index("y"), lax.axis_index("z_lo")
    return 2 * y + z_lo, lax.axis_index("core"), y, z_lo


def route_body(
    routes, logits, tokens, up, own, other, combine, far_up, columns, chosen_routes, raw, sems
):
    where = position_of()
    top, count = routes.shape
    slots, narrow = 2 * CHIPS * CAP, own.shape[2]
    half = far_up.shape[1]
    far_start = pl.multiple_of((1 - where[3]) * half, LANES)
    start = pl.multiple_of(where[0] * narrow, LANES)
    loads = [
        pltpu.make_async_copy(routes, chosen_routes, sems.at[0]),
        pltpu.make_async_copy(logits, raw, sems.at[1]),
        pltpu.make_async_copy(tokens.at[:, pl.ds(start, narrow)], columns, sems.at[2]),
        pltpu.make_async_copy(up.at[:, pl.ds(far_start, half)], far_up, sems.at[3]),
    ]
    for load in loads:
        load.start()
    for load in loads[:2]:
        load.wait()
    named = chosen_routes[...] ^ where[1]
    score = 1.0 / (1.0 + jnp.exp(-raw[...]))
    weight = SCALE * score / jnp.sum(score, axis=0, keepdims=True)
    slot = lax.broadcasted_iota(jnp.int32, (slots, count), 0)
    expert, place = slot // CAP, (slot % CAP).astype(F32)
    hits = jnp.zeros((slots, count), F32)
    shares = jnp.zeros((slots, count), F32)
    for k in range(top):
        hit = named[k : k + 1, :] == expert
        hits = jnp.where(hit, 1.0, hits)
        shares = jnp.where(hit, weight[k : k + 1, :], shares)
    earlier = (
        lax.broadcasted_iota(jnp.int32, (count, count), 0)
        < lax.broadcasted_iota(jnp.int32, (count, count), 1)
    ).astype(F32)
    position = jnp.dot(hits.astype(BF), earlier.astype(BF), preferred_element_type=F32)
    chosen = (hits > 0.5) & (position == place)
    picker = jnp.where(chosen, 1.0, 0.0).astype(BF)
    loads[2].wait()
    picked = jnp.dot(picker, columns[...], preferred_element_type=F32)
    picked = picked.reshape(CHIPS, 2, CAP, narrow)
    own[...] = picked[:, 0].astype(BF)
    other[...] = picked[:, 1].astype(BF)
    exact = jnp.where(chosen, shares, 0.0)
    high = exact.astype(BF)
    rest = exact - high.astype(F32)
    middle = rest.astype(BF)
    for k, term in enumerate((high, middle, (rest - middle.astype(F32)).astype(BF))):
        paired = term.astype(F32).reshape(CHIPS, 2, CAP, count)
        for r in range(2):
            combine[k, r] = paired[:, r].reshape(CHIPS * CAP, count).astype(BF)
    loads[3].wait()


def route(routes, logits, tokens, up):
    count = tokens.shape[0]
    narrow, units = up.shape
    slots = 2 * CHIPS * CAP
    return kernel(
        route_body,
        "route",
        4,
        out_shape=(
            pltpu.VMEM((CHIPS, CAP, narrow), BF),
            pltpu.VMEM((CHIPS, CAP, narrow), BF),
            pltpu.VMEM((3, 2, slots // 2, count), BF),
            pltpu.VMEM((narrow, units // 2), BF),
        ),
        in_specs=[HB, HB, HB, HB],
        out_specs=(VM, VM, VM, VM),
        scratch_shapes=[
            pltpu.VMEM((count, narrow), BF),
            pltpu.VMEM(routes.shape, jnp.int32),
            pltpu.VMEM(logits.shape, F32),
            pltpu.SemaphoreType.DMA((4,)),
        ],
    )(in_hbm(routes), in_hbm(logits), in_hbm(tokens), in_hbm(up))


def split_body(arrived, out):
    out[...] = arrived[:, 1]


def split(arrived):
    chips, _, cap, narrow = arrived.shape
    return kernel(
        split_body,
        "split",
        4,
        out_shape=pltpu.VMEM((chips, cap, narrow), BF),
        in_specs=[VM],
        out_specs=VM,
    )(in_vmem(arrived))


def merge_body(own, other, out):
    out[:, 0] = own[...]
    out[:, 1] = other[...]


def merge(own, other):
    chips, cap, narrow = own.shape
    return kernel(
        merge_body,
        "merge",
        4,
        out_shape=pltpu.VMEM((chips, 2, cap, narrow), BF),
        in_specs=[VM, VM],
        out_specs=VM,
    )(in_vmem(own), in_vmem(other))


def replaced_body(arrived, other, out):
    out[:, 0] = arrived[:, 0]
    out[:, 1] = other[...]


def replaced(arrived, other):
    return kernel(
        replaced_body,
        "replaced",
        4,
        out_shape=pltpu.VMEM(arrived.shape, BF),
        in_specs=[VM, VM],
        out_specs=VM,
    )(in_vmem(arrived), in_vmem(other))


def gathered_rows(arrived):
    chips, _, cap, narrow = arrived.shape
    return jnp.concatenate(
        [arrived[:, r].reshape(chips * cap, narrow) for r in range(2)], axis=0
    )


def multiply(where, rows, weights, outs, steps, held):
    for j, weight in enumerate(weights):
        result = jnp.dot(rows, weight, preferred_element_type=F32)
        for y in range(4):
            held[y, :, j * LANES : (j + 1) * LANES] = result[:, y * LANES : (y + 1) * LANES]
    for (dy, _), out in zip(steps, outs):
        out[...] = held[(where[2] + dy) % 4].astype(out.dtype)


def far_body(arrived, gate, far_up, *rest):
    where = position_of()
    *outs, held = rest
    rows = gathered_rows(arrived)
    half = far_up.shape[1]
    for parity in range(2):

        @pl.when(where[3] == parity)
        def _():
            start = (1 - parity) * half
            weights = gate[:, start : start + half], far_up[...]
            multiply(where, rows, weights, outs, FAR, held)


def near_body(arrived, gate, up, *rest):
    where = position_of()
    *outs, held = rest
    rows = gathered_rows(arrived)
    half = gate.shape[1] // 2
    for parity in range(2):

        @pl.when(where[3] == parity)
        def _():
            start = parity * half
            weights = gate[:, start : start + half], up[:, start : start + half]
            multiply(where, rows, weights, outs, NEAR, held)


def far_parts(arrived, gate, up):
    rows = 2 * CHIPS * CAP
    return kernel(
        far_body,
        "far",
        8,
        out_shape=[pltpu.VMEM((rows, 2 * LANES), kind) for _, kind in FAR],
        in_specs=[VM, VM, VM],
        out_specs=[VM] * 4,
        scratch_shapes=[pltpu.VMEM((4, rows, 2 * LANES), F32)],
    )(in_vmem(arrived), in_vmem(gate), in_vmem(up))


def near_parts(arrived, gate, up):
    rows = 2 * CHIPS * CAP
    return kernel(
        near_body,
        "near",
        8,
        out_shape=[pltpu.VMEM((rows, 2 * LANES), kind) for _, kind in NEAR],
        in_specs=[VM, VM, VM],
        out_specs=[VM] * 4,
        scratch_shapes=[pltpu.VMEM((4, rows, 2 * LANES), F32)],
    )(in_vmem(arrived), in_vmem(gate), in_vmem(up))


def total_of(parts):
    total = parts[0][...].astype(F32)
    for part in parts[1:]:
        total = total + part[...].astype(F32)
    return total


def sum_body(*refs):
    *parts, out = refs
    out[...] = total_of(parts).astype(BF)


def summed(parts):
    return kernel(
        sum_body,
        "sum",
        4,
        out_shape=pltpu.VMEM(parts[0].shape, BF),
        in_specs=[VM] * len(parts),
        out_specs=VM,
    )(*[in_vmem(part) for part in parts])


def hidden_body(*refs):
    *parts, out = refs
    total = total_of(parts)
    gate, up = total[:, :LANES], total[:, LANES:]
    hidden = (gate / (1.0 + jnp.exp(-gate)) * up).astype(BF)
    for k in range(out.shape[0]):
        out[k] = hidden


def hidden_units(parts):
    return kernel(
        hidden_body,
        "hidden",
        4,
        out_shape=pltpu.VMEM((8, parts[0].shape[0], LANES), BF),
        in_specs=[VM] * len(parts),
        out_specs=VM,
    )(*[in_vmem(part) for part in parts])


def down_body(hidden, down, out):
    wide = jnp.concatenate([hidden[k] for k in range(8)], axis=1)
    result = lax.dot_general(
        wide, down[...], (((1,), (1,)), ((), ())), preferred_element_type=F32
    ).astype(BF)
    half = result.shape[0] // 2
    for r in range(2):
        out[:, r] = result[r * half : (r + 1) * half].reshape(CHIPS, CAP, result.shape[1])


def down_rows(hidden, down):
    return kernel(
        down_body,
        "down",
        8,
        out_shape=pltpu.VMEM((CHIPS, 2, CAP, down.shape[0]), BF),
        in_specs=[VM, VM],
        out_specs=VM,
    )(in_vmem(hidden), in_vmem(down))


def weighted(combine, r, rows):
    rows = rows.reshape(CHIPS * CAP, rows.shape[2])
    high, middle, low = [
        lax.dot_general(
            combine[k, r], rows, (((0,), (0,)), ((), ())), preferred_element_type=F32
        )
        for k in range(3)
    ]
    return high + (middle + low)


def own_mix_body(back, combine, out):
    out[...] = weighted(combine, 0, back[:, 0])


def own_mix(back, combine):
    return kernel(
        own_mix_body,
        "own_mix",
        4,
        out_shape=pltpu.VMEM((combine.shape[3], back.shape[3]), F32),
        in_specs=[VM, VM],
        out_specs=VM,
    )(in_vmem(back), in_vmem(combine))


def mix_body(partial, other, combine, out):
    out[...] = (partial[...] + weighted(combine, 1, other[...])).astype(BF)


def mix(partial, other, combine):
    return kernel(
        mix_body,
        "mix",
        4,
        out_shape=jax.ShapeDtypeStruct(partial.shape, BF),
        in_specs=[VM, VM, VM],
        out_specs=VM,
    )(in_vmem(partial), in_vmem(other), in_vmem(combine))


def shards(tokens, routes, route_logits, gate_weight, up_weight, down_weight):
    chips = ("x", "z_hi")
    narrow = gate_weight.shape[1]
    swap = [(0, 1), (1, 0)]
    gate, up, down = gate_weight[0], up_weight[0], down_weight[0]

    own, other, combine, far_up = route(routes.T, route_logits.T, tokens, up)
    rows = merge(own, other).reshape(CHIPS, 2 * CAP, narrow)
    arrived = lax.all_to_all(
        rows, chips, split_axis=0, concat_axis=0, tiled=True
    ).reshape(CHIPS, 2, CAP, narrow)
    other = lax.ppermute(split(arrived), "core", swap)
    arrived = replaced(arrived, other)

    def along_y(array, dy):
        return lax.ppermute(array, "y", [(j, (j + dy) % 4) for j in range(4)])

    def across_z(array):
        return lax.ppermute(array, "z_lo", swap)

    far2, far1, far3, far0 = far_parts(arrived, gate, far_up)
    crossed = across_z(far2)
    far1, far3 = along_y(far1, 1), along_y(far3, 3)
    near1, near3, near2, near0 = near_parts(arrived, gate, up)
    near1, near3 = along_y(near1, 1), along_y(near3, 3)
    near2 = along_y(summed([near2, crossed]), 2)
    relayed = across_z(summed([far0, far1, far3]))
    copies = hidden_units([near0, near1, near3, near2, relayed])
    hidden = lax.all_to_all(copies, ("z_lo", "y"), split_axis=0, concat_axis=0, tiled=True)
    back = lax.all_to_all(
        down_rows(hidden, down).reshape(CHIPS, 2 * CAP, narrow),
        chips, split_axis=0, concat_axis=0, tiled=True,
    ).reshape(CHIPS, 2, CAP, narrow)
    other = lax.ppermute(split(back), "core", swap)
    return mix(own_mix(back, combine), other, combine)


def solution(mesh):
    wide = Mesh(mesh.devices.reshape(4, 4, 2, 4, 2), ("x", "z_hi", "core", "y", "z_lo"))
    expert, tensor = ("x", "z_hi", "core"), ("y", "z_lo")
    return jax.shard_map(
        shards,
        mesh=wide,
        in_specs=(
            P(expert, None),
            P(expert, None),
            P(expert, None),
            P(expert, tensor, None),
            P(expert, tensor, None),
            P(expert, tensor, None),
        ),
        out_specs=P(expert, tensor),
        check_vma=False,
    )
```

```python
import jax
import jax.numpy as jnp
from jax import lax
from jax.experimental import pallas as pl
from jax.experimental.pallas import tpu as pltpu
from jax.sharding import Mesh, PartitionSpec as P


SCALE = 2.5
CHIPS = 16
CAP = 8
LANES = 128
BF = jnp.bfloat16
F32 = jnp.float32
FAR = ((2, BF), (1, BF), (3, BF), (0, F32))
NEAR = ((1, BF), (3, BF), (2, F32), (0, F32))

VM = pl.BlockSpec(memory_space=pltpu.VMEM)
HB = pl.BlockSpec(memory_space=pltpu.HBM)
SM = pl.BlockSpec(memory_space=pltpu.SMEM)


def in_vmem(array):
    return pltpu.with_memory_space_constraint(array, pltpu.VMEM)


def in_hbm(array):
    return pltpu.with_memory_space_constraint(array, pltpu.HBM)


def kernel(body, name, mib, **settings):
    return pl.pallas_call(
        body,
        compiler_params=pltpu.CompilerParams(vmem_limit_bytes=mib << 20),
        name=name,
        **settings,
    )


def position_of():
    y, z_lo = lax.axis_index("y"), lax.axis_index("z_lo")
    return 2 * y + z_lo, lax.axis_index("core"), y, z_lo


def route_body(
    routes, logits, tokens, up, own, other, combine, far_up, columns, chosen_routes, raw, sems
):
    where = position_of()
    top, count = routes.shape
    slots, narrow = 2 * CHIPS * CAP, own.shape[2]
    half = far_up.shape[1]
    far_start = pl.multiple_of((1 - where[3]) * half, LANES)
    start = pl.multiple_of(where[0] * narrow, LANES)
    loads = [
        pltpu.make_async_copy(routes, chosen_routes, sems.at[0]),
        pltpu.make_async_copy(logits, raw, sems.at[1]),
        pltpu.make_async_copy(tokens.at[:, pl.ds(start, narrow)], columns, sems.at[2]),
        pltpu.make_async_copy(up.at[:, pl.ds(far_start, half)], far_up, sems.at[3]),
    ]
    for load in loads:
        load.start()
    for load in loads[:2]:
        load.wait()
    named = chosen_routes[...] ^ where[1]
    score = 1.0 / (1.0 + jnp.exp(-raw[...]))
    weight = SCALE * score / jnp.sum(score, axis=0, keepdims=True)
    slot = lax.broadcasted_iota(jnp.int32, (slots, count), 0)
    expert, place = slot // CAP, (slot % CAP).astype(F32)
    hits = jnp.zeros((slots, count), F32)
    shares = jnp.zeros((slots, count), F32)
    for k in range(top):
        hit = named[k : k + 1, :] == expert
        hits = jnp.where(hit, 1.0, hits)
        shares = jnp.where(hit, weight[k : k + 1, :], shares)
    earlier = (
        lax.broadcasted_iota(jnp.int32, (count, count), 0)
        < lax.broadcasted_iota(jnp.int32, (count, count), 1)
    ).astype(F32)
    position = jnp.dot(hits.astype(BF), earlier.astype(BF), preferred_element_type=F32)
    chosen = (hits > 0.5) & (position == place)
    picker = jnp.where(chosen, 1.0, 0.0).astype(BF)
    loads[2].wait()
    picked = jnp.dot(picker, columns[...], preferred_element_type=F32)
    picked = picked.reshape(CHIPS, 2, CAP, narrow)
    own[...] = picked[:, 0].astype(BF)
    other[...] = picked[:, 1].astype(BF)
    exact = jnp.where(chosen, shares, 0.0)
    high = exact.astype(BF)
    rest = exact - high.astype(F32)
    middle = rest.astype(BF)
    for k, term in enumerate((high, middle, (rest - middle.astype(F32)).astype(BF))):
        paired = term.astype(F32).reshape(CHIPS, 2, CAP, count)
        for r in range(2):
            combine[k, r] = paired[:, r].reshape(CHIPS * CAP, count).astype(BF)
    loads[3].wait()


def route(routes, logits, tokens, up):
    count = tokens.shape[0]
    narrow, units = up.shape
    slots = 2 * CHIPS * CAP
    return kernel(
        route_body,
        "route",
        4,
        out_shape=(
            pltpu.VMEM((CHIPS, CAP, narrow), BF),
            pltpu.VMEM((CHIPS, CAP, narrow), BF),
            pltpu.VMEM((3, 2, slots // 2, count), BF),
            pltpu.VMEM((narrow, units // 2), BF),
        ),
        in_specs=[HB, HB, HB, HB],
        out_specs=(VM, VM, VM, VM),
        scratch_shapes=[
            pltpu.VMEM((count, narrow), BF),
            pltpu.VMEM(routes.shape, jnp.int32),
            pltpu.VMEM(logits.shape, F32),
            pltpu.SemaphoreType.DMA((4,)),
        ],
    )(in_hbm(routes), in_hbm(logits), in_hbm(tokens), in_hbm(up))


def split_body(arrived, out):
    out[...] = arrived[:, 1]


def split(arrived):
    chips, _, cap, narrow = arrived.shape
    return kernel(
        split_body,
        "split",
        4,
        out_shape=pltpu.VMEM((chips, cap, narrow), BF),
        in_specs=[VM],
        out_specs=VM,
    )(in_vmem(arrived))


def merge_body(own, other, out):
    out[:, 0] = own[...]
    out[:, 1] = other[...]


def merge(own, other):
    chips, cap, narrow = own.shape
    return kernel(
        merge_body,
        "merge",
        4,
        out_shape=pltpu.VMEM((chips, 2, cap, narrow), BF),
        in_specs=[VM, VM],
        out_specs=VM,
    )(in_vmem(own), in_vmem(other))


def own_rows(arrived):
    chips, _, cap, narrow = arrived.shape
    return arrived[:, 0].reshape(chips * cap, narrow)


def flat_rows(other):
    chips, cap, narrow = other.shape
    return other[...].reshape(chips * cap, narrow)


def multiply(where, rows, weights, outs, steps, held):
    for j, weight in enumerate(weights):
        result = jnp.dot(rows, weight, preferred_element_type=F32)
        for y in range(4):
            held[y, :, j * LANES : (j + 1) * LANES] = result[:, y * LANES : (y + 1) * LANES]
    for (dy, _), out in zip(steps, outs):
        out[...] = held[(where[2] + dy) % 4].astype(out.dtype)


def far_weights(where, gate, far_up, use):
    half = far_up.shape[1]
    for parity in range(2):

        @pl.when(where[3] == parity)
        def _():
            start = (1 - parity) * half
            use((gate[:, start : start + half], far_up[...]))


def own_far_body(arrived, gate, far_up, *rest):
    where = position_of()
    *outs, held = rest
    rows = own_rows(arrived)
    far_weights(
        where, gate, far_up, lambda pair: multiply(where, rows, pair, outs, FAR, held)
    )


def far_body(*refs):
    where = position_of()
    *owns, other, gate, far_up, out0, out1, out2, out3, held = refs
    outs = out0, out1, out2, out3
    rows = flat_rows(other)
    half = rows.shape[0]
    for own, out in zip(owns, outs):
        out[:half] = own[...]
    lower = [out.at[half:] for out in outs]
    far_weights(
        where, gate, far_up, lambda pair: multiply(where, rows, pair, lower, FAR, held)
    )


def near_body(arrived, other, gate, up, *rest):
    where = position_of()
    *outs, held = rest
    rows = jnp.concatenate([own_rows(arrived), flat_rows(other)], axis=0)
    half = gate.shape[1] // 2
    for parity in range(2):

        @pl.when(where[3] == parity)
        def _():
            start = parity * half
            weights = gate[:, start : start + half], up[:, start : start + half]
            multiply(where, rows, weights, outs, NEAR, held)


def own_far_parts(arrived, gate, far_up):
    rows = CHIPS * CAP
    return kernel(
        own_far_body,
        "own_far",
        8,
        out_shape=[pltpu.VMEM((rows, 2 * LANES), kind) for _, kind in FAR],
        in_specs=[VM, VM, VM],
        out_specs=[VM] * 4,
        scratch_shapes=[pltpu.VMEM((4, rows, 2 * LANES), F32)],
    )(in_vmem(arrived), in_vmem(gate), in_vmem(far_up))


def far_parts(owns, other, gate, far_up):
    rows = CHIPS * CAP
    return kernel(
        far_body,
        "far",
        8,
        out_shape=[pltpu.VMEM((2 * rows, 2 * LANES), kind) for _, kind in FAR],
        in_specs=[VM] * 7,
        out_specs=[VM] * 4,
        scratch_shapes=[pltpu.VMEM((4, rows, 2 * LANES), F32)],
    )(*[in_vmem(own) for own in owns], in_vmem(other), in_vmem(gate), in_vmem(far_up))


def near_parts(arrived, other, gate, up):
    rows = 2 * CHIPS * CAP
    return kernel(
        near_body,
        "near",
        8,
        out_shape=[pltpu.VMEM((rows, 2 * LANES), kind) for _, kind in NEAR],
        in_specs=[VM, VM, VM, VM],
        out_specs=[VM] * 4,
        scratch_shapes=[pltpu.VMEM((4, rows, 2 * LANES), F32)],
    )(in_vmem(arrived), in_vmem(other), in_vmem(gate), in_vmem(up))


def total_of(parts):
    total = parts[0][...].astype(F32)
    for part in parts[1:]:
        total = total + part[...].astype(F32)
    return total


def sum_body(*refs):
    *parts, out = refs
    out[...] = total_of(parts).astype(BF)


def summed(parts):
    return kernel(
        sum_body,
        "sum",
        4,
        out_shape=pltpu.VMEM(parts[0].shape, BF),
        in_specs=[VM] * len(parts),
        out_specs=VM,
    )(*[in_vmem(part) for part in parts])


def hidden_body(*refs):
    *parts, out = refs
    total = total_of(parts)
    gate, up = total[:, :LANES], total[:, LANES:]
    hidden = (gate / (1.0 + jnp.exp(-gate)) * up).astype(BF)
    for k in range(out.shape[0]):
        out[k] = hidden


def hidden_units(parts):
    return kernel(
        hidden_body,
        "hidden",
        4,
        out_shape=pltpu.VMEM((8, parts[0].shape[0], LANES), BF),
        in_specs=[VM] * len(parts),
        out_specs=VM,
    )(*[in_vmem(part) for part in parts])


def down_body(hidden, down, out):
    wide = jnp.concatenate([hidden[k] for k in range(8)], axis=1)
    result = lax.dot_general(
        wide, down[...], (((1,), (1,)), ((), ())), preferred_element_type=F32
    ).astype(BF)
    half = result.shape[0] // 2
    for r in range(2):
        out[:, r] = result[r * half : (r + 1) * half].reshape(CHIPS, CAP, result.shape[1])


def down_rows(hidden, down):
    return kernel(
        down_body,
        "down",
        8,
        out_shape=pltpu.VMEM((CHIPS, 2, CAP, down.shape[0]), BF),
        in_specs=[VM, VM],
        out_specs=VM,
    )(in_vmem(hidden), in_vmem(down))


def weighted(combine, r, rows):
    rows = rows.reshape(CHIPS * CAP, rows.shape[2])
    high, middle, low = [
        lax.dot_general(
            combine[k, r], rows, (((0,), (0,)), ((), ())), preferred_element_type=F32
        )
        for k in range(3)
    ]
    return high + (middle + low)


def own_mix_body(back, combine, out):
    out[...] = weighted(combine, 0, back[:, 0])


def own_mix(back, combine):
    return kernel(
        own_mix_body,
        "own_mix",
        4,
        out_shape=pltpu.VMEM((combine.shape[3], back.shape[3]), F32),
        in_specs=[VM, VM],
        out_specs=VM,
    )(in_vmem(back), in_vmem(combine))


def mix_body(partial, other, combine, out):
    out[...] = (partial[...] + weighted(combine, 1, other[...])).astype(BF)


def mix(partial, other, combine):
    return kernel(
        mix_body,
        "mix",
        4,
        out_shape=jax.ShapeDtypeStruct(partial.shape, BF),
        in_specs=[VM, VM, VM],
        out_specs=VM,
    )(in_vmem(partial), in_vmem(other), in_vmem(combine))


def shards(tokens, routes, route_logits, gate_weight, up_weight, down_weight):
    chips = ("x", "z_hi")
    narrow = gate_weight.shape[1]
    swap = [(0, 1), (1, 0)]
    gate, up, down = gate_weight[0], up_weight[0], down_weight[0]

    own, other, combine, far_up = route(routes.T, route_logits.T, tokens, up)
    rows = merge(own, other).reshape(CHIPS, 2 * CAP, narrow)
    arrived = lax.all_to_all(
        rows, chips, split_axis=0, concat_axis=0, tiled=True
    ).reshape(CHIPS, 2, CAP, narrow)
    other = lax.ppermute(split(arrived), "core", swap)
    owns = own_far_parts(arrived, gate, far_up)

    def along_y(array, dy):
        return lax.ppermute(array, "y", [(j, (j + dy) % 4) for j in range(4)])

    def across_z(array):
        return lax.ppermute(array, "z_lo", swap)

    far2, far1, far3, far0 = far_parts(owns, other, gate, far_up)
    crossed = across_z(far2)
    far1, far3 = along_y(far1, 1), along_y(far3, 3)
    near1, near3, near2, near0 = near_parts(arrived, other, gate, up)
    near1, near3 = along_y(near1, 1), along_y(near3, 3)
    near2 = along_y(summed([near2, crossed]), 2)
    relayed = across_z(summed([far0, far1, far3]))
    copies = hidden_units([near0, near1, near3, near2, relayed])
    hidden = lax.all_to_all(copies, ("z_lo", "y"), split_axis=0, concat_axis=0, tiled=True)
    back = lax.all_to_all(
        down_rows(hidden, down).reshape(CHIPS, 2 * CAP, narrow),
        chips, split_axis=0, concat_axis=0, tiled=True,
    ).reshape(CHIPS, 2, CAP, narrow)
    other = lax.ppermute(split(back), "core", swap)
    return mix(own_mix(back, combine), other, combine)


def solution(mesh):
    wide = Mesh(mesh.devices.reshape(4, 4, 2, 4, 2), ("x", "z_hi", "core", "y", "z_lo"))
    expert, tensor = ("x", "z_hi", "core"), ("y", "z_lo")
    return jax.shard_map(
        shards,
        mesh=wide,
        in_specs=(
            P(expert, None),
            P(expert, None),
            P(expert, None),
            P(expert, tensor, None),
            P(expert, tensor, None),
            P(expert, tensor, None),
        ),
        out_specs=P(expert, tensor),
        check_vma=False,
    )
```

```python
import jax
import jax.numpy as jnp
from jax import lax
from jax.experimental import pallas as pl
from jax.experimental.pallas import tpu as pltpu
from jax.sharding import Mesh, PartitionSpec as P


SCALE = 2.5
CHIPS = 16
CAP = 8
LANES = 128
BF = jnp.bfloat16
F32 = jnp.float32
FAR = ((2, BF), (1, BF), (3, BF), (0, F32))
NEAR = ((1, BF), (3, BF), (2, F32), (0, F32))

VM = pl.BlockSpec(memory_space=pltpu.VMEM)
HB = pl.BlockSpec(memory_space=pltpu.HBM)
SM = pl.BlockSpec(memory_space=pltpu.SMEM)


def in_vmem(array):
    return pltpu.with_memory_space_constraint(array, pltpu.VMEM)


def in_hbm(array):
    return pltpu.with_memory_space_constraint(array, pltpu.HBM)


def kernel(body, name, mib, **settings):
    return pl.pallas_call(
        body,
        compiler_params=pltpu.CompilerParams(vmem_limit_bytes=mib << 20),
        name=name,
        **settings,
    )


def position_of():
    y, z_lo = lax.axis_index("y"), lax.axis_index("z_lo")
    return 2 * y + z_lo, lax.axis_index("core"), y, z_lo


def route_body(
    routes, logits, tokens, up, send, combine, far_up, columns, chosen_routes, raw, sems
):
    where = position_of()
    top, count = routes.shape
    slots, narrow = 2 * CHIPS * CAP, send.shape[3]
    half = far_up.shape[1]
    far_start = pl.multiple_of((1 - where[3]) * half, LANES)
    start = pl.multiple_of(where[0] * narrow, LANES)
    loads = [
        pltpu.make_async_copy(routes, chosen_routes, sems.at[0]),
        pltpu.make_async_copy(logits, raw, sems.at[1]),
        pltpu.make_async_copy(tokens.at[:, pl.ds(start, narrow)], columns, sems.at[2]),
        pltpu.make_async_copy(up.at[:, pl.ds(far_start, half)], far_up, sems.at[3]),
    ]
    for load in loads:
        load.start()
    for load in loads[:2]:
        load.wait()
    named = chosen_routes[...] ^ where[1]
    score = 1.0 / (1.0 + jnp.exp(-raw[...]))
    weight = SCALE * score / jnp.sum(score, axis=0, keepdims=True)
    slot = lax.broadcasted_iota(jnp.int32, (slots, count), 0)
    expert, place = slot // CAP, (slot % CAP).astype(F32)
    hits = jnp.zeros((slots, count), F32)
    shares = jnp.zeros((slots, count), F32)
    for k in range(top):
        hit = named[k : k + 1, :] == expert
        hits = jnp.where(hit, 1.0, hits)
        shares = jnp.where(hit, weight[k : k + 1, :], shares)
    earlier = (
        lax.broadcasted_iota(jnp.int32, (count, count), 0)
        < lax.broadcasted_iota(jnp.int32, (count, count), 1)
    ).astype(F32)
    position = jnp.dot(hits.astype(BF), earlier.astype(BF), preferred_element_type=F32)
    chosen = (hits > 0.5) & (position == place)
    picker = jnp.where(chosen, 1.0, 0.0).astype(BF)
    loads[2].wait()
    picked = jnp.dot(picker, columns[...], preferred_element_type=F32)
    picked = picked.reshape(CHIPS, 2, CAP, narrow)
    send[...] = picked.astype(BF)
    exact = jnp.where(chosen, shares, 0.0)
    high = exact.astype(BF)
    rest = exact - high.astype(F32)
    middle = rest.astype(BF)
    for k, term in enumerate((high, middle, (rest - middle.astype(F32)).astype(BF))):
        paired = term.astype(F32).reshape(CHIPS, 2, CAP, count)
        for r in range(2):
            combine[k, r] = paired[:, r].reshape(CHIPS * CAP, count).astype(BF)
    loads[3].wait()


def route(routes, logits, tokens, up):
    count = tokens.shape[0]
    narrow, units = up.shape
    slots = 2 * CHIPS * CAP
    return kernel(
        route_body,
        "route",
        4,
        out_shape=(
            pltpu.VMEM((CHIPS, 2, CAP, narrow), BF),
            pltpu.VMEM((3, 2, slots // 2, count), BF),
            pltpu.VMEM((narrow, units // 2), BF),
        ),
        in_specs=[HB, HB, HB, HB],
        out_specs=(VM, VM, VM),
        scratch_shapes=[
            pltpu.VMEM((count, narrow), BF),
            pltpu.VMEM(routes.shape, jnp.int32),
            pltpu.VMEM(logits.shape, F32),
            pltpu.SemaphoreType.DMA((4,)),
        ],
    )(in_hbm(routes), in_hbm(logits), in_hbm(tokens), in_hbm(up))


def split_body(arrived, out):
    out[...] = arrived[:, 1]


def split(arrived):
    chips, _, cap, narrow = arrived.shape
    return kernel(
        split_body,
        "split",
        4,
        out_shape=pltpu.VMEM((chips, cap, narrow), BF),
        in_specs=[VM],
        out_specs=VM,
    )(in_vmem(arrived))


def own_rows(arrived):
    chips, _, cap, narrow = arrived.shape
    return arrived[:, 0].reshape(chips * cap, narrow)


def flat_rows(other):
    chips, cap, narrow = other.shape
    return other[...].reshape(chips * cap, narrow)


def multiply(where, rows, weights, outs, steps, held):
    for j, weight in enumerate(weights):
        result = jnp.dot(rows, weight, preferred_element_type=F32)
        for y in range(4):
            held[y, :, j * LANES : (j + 1) * LANES] = result[:, y * LANES : (y + 1) * LANES]
    for (dy, _), out in zip(steps, outs):
        out[...] = held[where[2] ^ dy].astype(out.dtype)


def far_weights(where, gate, far_up, use):
    half = far_up.shape[1]
    for parity in range(2):

        @pl.when(where[3] == parity)
        def _():
            start = (1 - parity) * half
            use((gate[:, start : start + half], far_up[...]))


def own_far_body(arrived, gate, far_up, *rest):
    where = position_of()
    *outs, held = rest
    rows = own_rows(arrived)
    far_weights(
        where, gate, far_up, lambda pair: multiply(where, rows, pair, outs, FAR, held)
    )


def far_body(*refs):
    where = position_of()
    *owns, other, gate, far_up, out0, out1, out2, out3, held = refs
    outs = out0, out1, out2, out3
    rows = flat_rows(other)
    half = rows.shape[0]
    for own, out in zip(owns, outs):
        out[:half] = own[...]
    lower = [out.at[half:] for out in outs]
    far_weights(
        where, gate, far_up, lambda pair: multiply(where, rows, pair, lower, FAR, held)
    )


def near_body(arrived, other, gate, up, *rest):
    where = position_of()
    *outs, held = rest
    rows = jnp.concatenate([own_rows(arrived), flat_rows(other)], axis=0)
    half = gate.shape[1] // 2
    for parity in range(2):

        @pl.when(where[3] == parity)
        def _():
            start = parity * half
            weights = gate[:, start : start + half], up[:, start : start + half]
            multiply(where, rows, weights, outs, NEAR, held)


def own_far_parts(arrived, gate, far_up):
    rows = CHIPS * CAP
    return kernel(
        own_far_body,
        "own_far",
        8,
        out_shape=[pltpu.VMEM((rows, 2 * LANES), kind) for _, kind in FAR],
        in_specs=[VM, VM, VM],
        out_specs=[VM] * 4,
        scratch_shapes=[pltpu.VMEM((4, rows, 2 * LANES), F32)],
    )(in_vmem(arrived), in_vmem(gate), in_vmem(far_up))


def far_parts(owns, other, gate, far_up):
    rows = CHIPS * CAP
    return kernel(
        far_body,
        "far",
        8,
        out_shape=[pltpu.VMEM((2 * rows, 2 * LANES), kind) for _, kind in FAR],
        in_specs=[VM] * 7,
        out_specs=[VM] * 4,
        scratch_shapes=[pltpu.VMEM((4, rows, 2 * LANES), F32)],
    )(*[in_vmem(own) for own in owns], in_vmem(other), in_vmem(gate), in_vmem(far_up))


def near_parts(arrived, other, gate, up):
    rows = 2 * CHIPS * CAP
    return kernel(
        near_body,
        "near",
        8,
        out_shape=[pltpu.VMEM((rows, 2 * LANES), kind) for _, kind in NEAR],
        in_specs=[VM, VM, VM, VM],
        out_specs=[VM] * 4,
        scratch_shapes=[pltpu.VMEM((4, rows, 2 * LANES), F32)],
    )(in_vmem(arrived), in_vmem(other), in_vmem(gate), in_vmem(up))


def total_of(parts):
    total = parts[0][...].astype(F32)
    for part in parts[1:]:
        total = total + part[...].astype(F32)
    return total


def sum_body(*refs):
    *parts, out = refs
    out[...] = total_of(parts).astype(BF)


def summed(parts):
    return kernel(
        sum_body,
        "sum",
        4,
        out_shape=pltpu.VMEM(parts[0].shape, BF),
        in_specs=[VM] * len(parts),
        out_specs=VM,
    )(*[in_vmem(part) for part in parts])


def hidden_body(*refs):
    *parts, out = refs
    total = total_of(parts)
    gate, up = total[:, :LANES], total[:, LANES:]
    hidden = (gate / (1.0 + jnp.exp(-gate)) * up).astype(BF)
    for k in range(out.shape[0]):
        out[k] = hidden


def hidden_units(parts):
    return kernel(
        hidden_body,
        "hidden",
        4,
        out_shape=pltpu.VMEM((8, parts[0].shape[0], LANES), BF),
        in_specs=[VM] * len(parts),
        out_specs=VM,
    )(*[in_vmem(part) for part in parts])


def down_body(hidden, down, out):
    wide = jnp.concatenate([hidden[k] for k in range(8)], axis=1)
    result = lax.dot_general(
        wide, down[...], (((1,), (1,)), ((), ())), preferred_element_type=F32
    ).astype(BF)
    half = result.shape[0] // 2
    for r in range(2):
        out[:, r] = result[r * half : (r + 1) * half].reshape(CHIPS, CAP, result.shape[1])


def down_rows(hidden, down):
    return kernel(
        down_body,
        "down",
        8,
        out_shape=pltpu.VMEM((CHIPS, 2, CAP, down.shape[0]), BF),
        in_specs=[VM, VM],
        out_specs=VM,
    )(in_vmem(hidden), in_vmem(down))


def weighted(combine, r, rows):
    rows = rows.reshape(CHIPS * CAP, rows.shape[2])
    high, middle, low = [
        lax.dot_general(
            combine[k, r], rows, (((0,), (0,)), ((), ())), preferred_element_type=F32
        )
        for k in range(3)
    ]
    return high + (middle + low)


def own_mix_body(back, combine, out):
    out[...] = weighted(combine, 0, back[:, 0])


def own_mix(back, combine):
    return kernel(
        own_mix_body,
        "own_mix",
        4,
        out_shape=pltpu.VMEM((combine.shape[3], back.shape[3]), F32),
        in_specs=[VM, VM],
        out_specs=VM,
    )(in_vmem(back), in_vmem(combine))


def mix_body(partial, other, combine, out):
    out[...] = (partial[...] + weighted(combine, 1, other[...])).astype(BF)


def mix(partial, other, combine):
    return kernel(
        mix_body,
        "mix",
        4,
        out_shape=jax.ShapeDtypeStruct(partial.shape, BF),
        in_specs=[VM, VM, VM],
        out_specs=VM,
    )(in_vmem(partial), in_vmem(other), in_vmem(combine))


def shards(tokens, routes, route_logits, gate_weight, up_weight, down_weight):
    chips = ("x", "z_hi")
    narrow = gate_weight.shape[1]
    swap = [(0, 1), (1, 0)]
    gate, up, down = gate_weight[0], up_weight[0], down_weight[0]

    send, combine, far_up = route(routes.T, route_logits.T, tokens, up)
    rows = send.reshape(CHIPS, 2 * CAP, narrow)
    arrived = lax.all_to_all(
        rows, chips, split_axis=0, concat_axis=0, tiled=True
    ).reshape(CHIPS, 2, CAP, narrow)
    other = lax.ppermute(split(arrived), "core", swap)
    owns = own_far_parts(arrived, gate, far_up)

    def along_y(array, dy):
        return lax.ppermute(array, "y", [(j, j ^ dy) for j in range(4)])

    def across_z(array):
        return lax.ppermute(array, "z_lo", swap)

    far2, far1, far3, far0 = far_parts(owns, other, gate, far_up)
    crossed = across_z(far2)
    far1, far3 = along_y(far1, 1), along_y(far3, 3)
    near1, near3, near2, near0 = near_parts(arrived, other, gate, up)
    near1, near3 = along_y(near1, 1), along_y(near3, 3)
    near2 = along_y(summed([near2, crossed]), 2)
    relayed = across_z(summed([far0, far1, far3]))
    copies = hidden_units([near0, near1, near3, near2, relayed])
    hidden = lax.all_to_all(copies, ("z_lo", "y"), split_axis=0, concat_axis=0, tiled=True)
    back = lax.all_to_all(
        down_rows(hidden, down).reshape(CHIPS, 2 * CAP, narrow),
        chips, split_axis=0, concat_axis=0, tiled=True,
    ).reshape(CHIPS, 2, CAP, narrow)
    other = lax.ppermute(split(back), "core", swap)
    return mix(own_mix(back, combine), other, combine)


def solution(mesh):
    wide = Mesh(mesh.devices.reshape(4, 4, 2, 4, 2), ("x", "z_hi", "core", "y", "z_lo"))
    expert, tensor = ("x", "z_hi", "core"), ("y", "z_lo")
    return jax.shard_map(
        shards,
        mesh=wide,
        in_specs=(
            P(expert, None),
            P(expert, None),
            P(expert, None),
            P(expert, tensor, None),
            P(expert, tensor, None),
            P(expert, tensor, None),
        ),
        out_specs=P(expert, tensor),
        check_vma=False,
    )
```

```python
import jax
import jax.numpy as jnp
from jax import lax
from jax.experimental import pallas as pl
from jax.experimental.pallas import tpu as pltpu
from jax.sharding import Mesh, PartitionSpec as P


SCALE = 2.5
CHIPS = 16
CAP = 8
LANES = 128
BF = jnp.bfloat16
F32 = jnp.float32
FAR = ((2, BF), (1, BF), (3, BF), (0, F32))
NEAR = ((1, BF), (3, BF), (2, F32), (0, F32))

VM = pl.BlockSpec(memory_space=pltpu.VMEM)
HB = pl.BlockSpec(memory_space=pltpu.HBM)
SM = pl.BlockSpec(memory_space=pltpu.SMEM)


def in_vmem(array):
    return pltpu.with_memory_space_constraint(array, pltpu.VMEM)


def in_hbm(array):
    return pltpu.with_memory_space_constraint(array, pltpu.HBM)


def kernel(body, name, mib, **settings):
    return pl.pallas_call(
        body,
        compiler_params=pltpu.CompilerParams(vmem_limit_bytes=mib << 20),
        name=name,
        **settings,
    )


def position_of():
    y, z_lo = lax.axis_index("y"), lax.axis_index("z_lo")
    return 2 * y + z_lo, lax.axis_index("core"), y, z_lo


def route_body(
    routes, logits, tokens, up, send, combine, far_up, columns, chosen_routes, raw, sems
):
    where = position_of()
    top, count = routes.shape
    slots, narrow = 2 * CHIPS * CAP, send.shape[3]
    half = far_up.shape[1]
    far_start = pl.multiple_of((1 - where[3]) * half, LANES)
    start = pl.multiple_of(where[0] * narrow, LANES)
    loads = [
        pltpu.make_async_copy(routes, chosen_routes, sems.at[0]),
        pltpu.make_async_copy(logits, raw, sems.at[1]),
        pltpu.make_async_copy(tokens.at[:, pl.ds(start, narrow)], columns, sems.at[2]),
        pltpu.make_async_copy(up.at[:, pl.ds(far_start, half)], far_up, sems.at[3]),
    ]
    for load in loads:
        load.start()
    for load in loads[:2]:
        load.wait()
    named = chosen_routes[...] ^ where[1]
    score = 1.0 / (1.0 + jnp.exp(-raw[...]))
    weight = SCALE * score / jnp.sum(score, axis=0, keepdims=True)
    slot = lax.broadcasted_iota(jnp.int32, (slots, count), 0)
    expert, place = slot // CAP, (slot % CAP).astype(F32)
    hits = jnp.zeros((slots, count), F32)
    shares = jnp.zeros((slots, count), F32)
    for k in range(top):
        hit = named[k : k + 1, :] == expert
        hits = jnp.where(hit, 1.0, hits)
        shares = jnp.where(hit, weight[k : k + 1, :], shares)
    earlier = (
        lax.broadcasted_iota(jnp.int32, (count, count), 0)
        < lax.broadcasted_iota(jnp.int32, (count, count), 1)
    ).astype(F32)
    position = jnp.dot(hits.astype(BF), earlier.astype(BF), preferred_element_type=F32)
    chosen = (hits > 0.5) & (position == place)
    picker = jnp.where(chosen, 1.0, 0.0).astype(BF)
    loads[2].wait()
    picked = jnp.dot(picker, columns[...], preferred_element_type=F32)
    picked = picked.reshape(CHIPS, 2, CAP, narrow)
    send[...] = picked.astype(BF)
    exact = jnp.where(chosen, shares, 0.0)
    high = exact.astype(BF)
    rest = exact - high.astype(F32)
    middle = rest.astype(BF)
    for k, term in enumerate((high, middle, (rest - middle.astype(F32)).astype(BF))):
        paired = term.astype(F32).reshape(CHIPS, 2, CAP, count)
        for r in range(2):
            combine[k, r] = paired[:, r].reshape(CHIPS * CAP, count).astype(BF)
    loads[3].wait()


def route(routes, logits, tokens, up):
    count = tokens.shape[0]
    narrow, units = up.shape
    slots = 2 * CHIPS * CAP
    return kernel(
        route_body,
        "route",
        4,
        out_shape=(
            pltpu.VMEM((CHIPS, 2, CAP, narrow), BF),
            pltpu.VMEM((3, 2, slots // 2, count), BF),
            pltpu.VMEM((narrow, units // 2), BF),
        ),
        in_specs=[HB, HB, HB, HB],
        out_specs=(VM, VM, VM),
        scratch_shapes=[
            pltpu.VMEM((count, narrow), BF),
            pltpu.VMEM(routes.shape, jnp.int32),
            pltpu.VMEM(logits.shape, F32),
            pltpu.SemaphoreType.DMA((4,)),
        ],
    )(in_hbm(routes), in_hbm(logits), in_hbm(tokens), in_hbm(up))


def split_body(arrived, out):
    out[...] = arrived[:, 1]


def split(arrived):
    chips, _, cap, narrow = arrived.shape
    return kernel(
        split_body,
        "split",
        4,
        out_shape=pltpu.VMEM((chips, cap, narrow), BF),
        in_specs=[VM],
        out_specs=VM,
    )(in_vmem(arrived))


def own_rows(arrived):
    chips, _, cap, narrow = arrived.shape
    return arrived[:, 0].reshape(chips * cap, narrow)


def flat_rows(other):
    chips, cap, narrow = other.shape
    return other[...].reshape(chips * cap, narrow)


def multiply(where, rows, weights, outs, steps, held):
    for j, weight in enumerate(weights):
        result = jnp.dot(rows, weight, preferred_element_type=F32)
        for y in range(4):
            held[y, :, j * LANES : (j + 1) * LANES] = result[:, y * LANES : (y + 1) * LANES]
    for (dy, _), out in zip(steps, outs):
        out[...] = held[(where[2] + dy) % 4].astype(out.dtype)


def far_weights(where, gate, far_up, use):
    half = far_up.shape[1]
    for parity in range(2):

        @pl.when(where[3] == parity)
        def _():
            start = (1 - parity) * half
            use((gate[:, start : start + half], far_up[...]))


def own_far_body(arrived, gate, far_up, *rest):
    where = position_of()
    *outs, held = rest
    rows = own_rows(arrived)
    far_weights(
        where, gate, far_up, lambda pair: multiply(where, rows, pair, outs, FAR, held)
    )


def far_body(*refs):
    where = position_of()
    *owns, other, gate, far_up, out0, out1, out2, out3, held = refs
    outs = out0, out1, out2, out3
    rows = flat_rows(other)
    half = rows.shape[0]
    for own, out in zip(owns, outs):
        out[:half] = own[...]
    lower = [out.at[half:] for out in outs]
    far_weights(
        where, gate, far_up, lambda pair: multiply(where, rows, pair, lower, FAR, held)
    )


def near_body(arrived, other, gate, up, *rest):
    where = position_of()
    *outs, held = rest
    rows = jnp.concatenate([own_rows(arrived), flat_rows(other)], axis=0)
    half = gate.shape[1] // 2
    for parity in range(2):

        @pl.when(where[3] == parity)
        def _():
            start = parity * half
            weights = gate[:, start : start + half], up[:, start : start + half]
            multiply(where, rows, weights, outs, NEAR, held)


def own_far_parts(arrived, gate, far_up):
    rows = CHIPS * CAP
    return kernel(
        own_far_body,
        "own_far",
        8,
        out_shape=[pltpu.VMEM((rows, 2 * LANES), kind) for _, kind in FAR],
        in_specs=[VM, VM, VM],
        out_specs=[VM] * 4,
        scratch_shapes=[pltpu.VMEM((4, rows, 2 * LANES), F32)],
    )(in_vmem(arrived), in_vmem(gate), in_vmem(far_up))


def far_parts(owns, other, gate, far_up):
    rows = CHIPS * CAP
    return kernel(
        far_body,
        "far",
        8,
        out_shape=[pltpu.VMEM((2 * rows, 2 * LANES), kind) for _, kind in FAR],
        in_specs=[VM] * 7,
        out_specs=[VM] * 4,
        scratch_shapes=[pltpu.VMEM((4, rows, 2 * LANES), F32)],
    )(*[in_vmem(own) for own in owns], in_vmem(other), in_vmem(gate), in_vmem(far_up))


def near_parts(arrived, other, gate, up):
    rows = 2 * CHIPS * CAP
    return kernel(
        near_body,
        "near",
        8,
        out_shape=[pltpu.VMEM((rows, 2 * LANES), kind) for _, kind in NEAR],
        in_specs=[VM, VM, VM, VM],
        out_specs=[VM] * 4,
        scratch_shapes=[pltpu.VMEM((4, rows, 2 * LANES), F32)],
    )(in_vmem(arrived), in_vmem(other), in_vmem(gate), in_vmem(up))


def total_of(parts):
    total = parts[0][...].astype(F32)
    for part in parts[1:]:
        total = total + part[...].astype(F32)
    return total


def sum_body(*refs):
    *parts, out = refs
    out[...] = total_of(parts).astype(BF)


def summed(parts):
    return kernel(
        sum_body,
        "sum",
        4,
        out_shape=pltpu.VMEM(parts[0].shape, BF),
        in_specs=[VM] * len(parts),
        out_specs=VM,
    )(*[in_vmem(part) for part in parts])


def hidden_body(*refs):
    *parts, out = refs
    total = total_of(parts)
    gate, up = total[:, :LANES], total[:, LANES:]
    hidden = (gate / (1.0 + jnp.exp(-gate)) * up).astype(BF)
    for k in range(out.shape[0]):
        out[k] = hidden


def hidden_units(parts):
    return kernel(
        hidden_body,
        "hidden",
        4,
        out_shape=pltpu.VMEM((8, parts[0].shape[0], LANES), BF),
        in_specs=[VM] * len(parts),
        out_specs=VM,
    )(*[in_vmem(part) for part in parts])


def down_body(hidden, down, out):
    wide = jnp.concatenate([hidden[k] for k in range(8)], axis=1)
    result = lax.dot_general(
        wide, down[...], (((1,), (1,)), ((), ())), preferred_element_type=F32
    ).astype(BF)
    half = result.shape[0] // 2
    for r in range(2):
        out[:, r] = result[r * half : (r + 1) * half].reshape(CHIPS, CAP, result.shape[1])


def down_rows(hidden, down):
    return kernel(
        down_body,
        "down",
        8,
        out_shape=pltpu.VMEM((CHIPS, 2, CAP, down.shape[0]), BF),
        in_specs=[VM, VM],
        out_specs=VM,
    )(in_vmem(hidden), in_vmem(down))


def weighted(combine, r, rows):
    rows = rows.reshape(CHIPS * CAP, rows.shape[2])
    high, middle, low = [
        lax.dot_general(
            combine[k, r], rows, (((0,), (0,)), ((), ())), preferred_element_type=F32
        )
        for k in range(3)
    ]
    return high + (middle + low)


def own_mix_body(back, combine, out):
    out[...] = weighted(combine, 0, back[:, 0])


def own_mix(back, combine):
    return kernel(
        own_mix_body,
        "own_mix",
        4,
        out_shape=pltpu.VMEM((combine.shape[3], back.shape[3]), F32),
        in_specs=[VM, VM],
        out_specs=VM,
    )(in_vmem(back), in_vmem(combine))


def mix_body(partial, other, combine, out):
    out[...] = (partial[...] + weighted(combine, 1, other[...])).astype(BF)


def mix(partial, other, combine):
    return kernel(
        mix_body,
        "mix",
        4,
        out_shape=jax.ShapeDtypeStruct(partial.shape, BF),
        in_specs=[VM, VM, VM],
        out_specs=VM,
    )(in_vmem(partial), in_vmem(other), in_vmem(combine))


def shards(tokens, routes, route_logits, gate_weight, up_weight, down_weight):
    chips = ("x", "z_hi")
    narrow = gate_weight.shape[1]
    swap = [(0, 1), (1, 0)]
    gate, up, down = gate_weight[0], up_weight[0], down_weight[0]

    send, combine, far_up = route(routes.T, route_logits.T, tokens, up)
    rows = send.reshape(CHIPS, 2 * CAP, narrow)
    arrived = lax.all_to_all(
        rows, chips, split_axis=0, concat_axis=0, tiled=True
    ).reshape(CHIPS, 2, CAP, narrow)
    other = lax.ppermute(split(arrived), "core", swap)
    owns = own_far_parts(arrived, gate, far_up)

    def along_y(array, dy):
        return lax.ppermute(array, "y", [(j, (j + dy) % 4) for j in range(4)])

    def across_z(array):
        return lax.ppermute(array, "z_lo", swap)

    far2, far1, far3, far0 = far_parts(owns, other, gate, far_up)
    crossed = across_z(far2)
    far1, far3 = along_y(far1, 1), along_y(far3, 3)
    near1, near3, near2, near0 = near_parts(arrived, other, gate, up)
    near1, near3 = along_y(near1, 1), along_y(near3, 3)
    near2 = along_y(summed([near2, crossed]), 2)
    relayed = across_z(summed([far0, far1, far3]))
    copies = hidden_units([near0, near1, near3, near2, relayed])
    hidden = lax.all_to_all(copies, ("z_lo", "y"), split_axis=0, concat_axis=0, tiled=True)
    back = lax.all_to_all(
        down_rows(hidden, down).reshape(CHIPS, 2 * CAP, narrow),
        chips, split_axis=0, concat_axis=0, tiled=True,
    ).reshape(CHIPS, 2, CAP, narrow)
    other = lax.ppermute(split(back), "core", swap)
    return mix(own_mix(back, combine), other, combine)


def solution(mesh):
    wide = Mesh(mesh.devices.reshape(4, 4, 2, 4, 2), ("x", "z_hi", "core", "y", "z_lo"))
    expert, tensor = ("x", "z_hi", "core"), ("y", "z_lo")
    return jax.shard_map(
        shards,
        mesh=wide,
        in_specs=(
            P(expert, None),
            P(expert, None),
            P(expert, None),
            P(expert, tensor, None),
            P(expert, tensor, None),
            P(expert, tensor, None),
        ),
        out_specs=P(expert, tensor),
        check_vma=False,
    )
```
